32 devices in a mesh: dp: 4 (over y, z), tp: 8 (over x, core).
Axes of the slice: x: 4, y: 2, z: 2, core: 2. Of those that a mesh axis runs over, the one named last changes fastest.
The devices are a block of a 4x4x8 slice.
Arguments:
- x_a: bfloat16 [2048, 3072], P(('dp', 'tp')), parts along dimension 0
- x_b: bfloat16 [2048, 3072], P(('dp', 'tp')), parts along dimension 0
- labels_a: int32 [2048], P(('dp', 'tp')), parts along dimension 0
- labels_b: int32 [2048], P(('dp', 'tp')), parts along dimension 0
- w_head: bfloat16 [3072, 49152], P(None, 'tp')
Outputs:
- output 1: float32 [8], P('dp'), parts along dimension 0
- output 2: bfloat16 [12288, 49152], P('dp', 'tp'), parts along dimension 0
- output 3: bfloat16 [2048, 3072], P(('dp', 'tp')), parts along dimension 0
- output 4: bfloat16 [2048, 3072], P(('dp', 'tp')), parts along dimension 0
There are 4 independent parts. The reference program is written for one: setup_inputs(seed, part) draws one part's arguments, and reference() takes and returns one part's arrays. A program takes and returns all parts, laid end to end along the dimension named above; an argument that names none is the same for every part.
All inputs are finite; a program needn't handle non-finite values.
Results may differ from the reference program's by a relative error of at most 0.001.
Values are sent between devices in bfloat16 or wider.
A program may use at most 768 MiB of HBM per device.

```python
import math
import jax
import jax.numpy as jnp
from jax import lax

TOKENS = 512
HIDDEN = 3072
VOCAB = 49152
VOCAB_SPLIT = 8


def draw_labels(label_key):
    value_key, first_key, gap_key = jax.random.split(label_key, 3)
    label_ids = jax.random.randint(value_key, (TOKENS,), 0, VOCAB, jnp.int32)
    first_pos = jax.random.randint(first_key, (), 0, TOKENS, jnp.int32)
    second_pos = (first_pos + jax.random.randint(gap_key, (), 1, TOKENS, jnp.int32)) % TOKENS
    return label_ids.at[first_pos].set(0).at[second_pos].set(VOCAB - 1)


def setup_inputs(seed: int = 0, part: int = 0) -> dict:
    part_key = jax.random.fold_in(jax.random.key(seed), part)
    key_xa, key_xb, key_la, key_lb = jax.random.split(part_key, 4)
    x_a = jax.random.normal(key_xa, (TOKENS, HIDDEN), jnp.float32).astype(jnp.bfloat16)
    x_b = jax.random.normal(key_xb, (TOKENS, HIDDEN), jnp.float32).astype(jnp.bfloat16)
    w_scale = 2.5 / math.sqrt(HIDDEN)
    w_head = (jax.random.normal(jax.random.key(seed + 1), (HIDDEN, VOCAB), jnp.float32) * w_scale).astype(jnp.bfloat16)
    return {"x_a": x_a, "x_b": x_b, "labels_a": draw_labels(key_la), "labels_b": draw_labels(key_lb), "w_head": w_head}


def reference(x_a, x_b, labels_a, labels_b, w_head):
    shard_cols = VOCAB // VOCAB_SPLIT
    w_blocks = w_head.reshape(HIDDEN, VOCAB_SPLIT, shard_cols).transpose(1, 0, 2)
    offsets = jnp.arange(VOCAB_SPLIT, dtype=jnp.int32) * shard_cols
    x_flat = jnp.concatenate([x_a, x_b], axis=0)
    label_flat = jnp.concatenate([labels_a, labels_b], axis=0)
    col_ids = jnp.arange(shard_cols, dtype=jnp.int32)[None, :]

    def block_stats(block_args):
        w_block, offset = block_args
        logits = jnp.dot(x_flat, w_block, preferred_element_type=jnp.float32)
        block_max = jnp.max(logits, axis=1)
        block_sum = jnp.sum(jnp.exp(logits - block_max[:, None]), axis=1)
        label_hit = col_ids == (label_flat - offset)[:, None]
        block_target = jnp.sum(jnp.where(label_hit, logits, 0.0), axis=1)
        return block_max, block_sum, block_target

    all_max, all_sum, all_target = lax.map(block_stats, (w_blocks, offsets))
    row_max = jnp.max(all_max, axis=0)
    row_sum = jnp.sum(all_sum * jnp.exp(all_max - row_max[None, :]), axis=0)
    target = jnp.sum(all_target, axis=0)
    loss_tok = row_max + jnp.log(row_sum) - target
    losses = jnp.stack([jnp.mean(loss_tok[:TOKENS]), jnp.mean(loss_tok[TOKENS:])])

    def block_grad(dx_acc, block_args):
        w_block, offset = block_args
        logits = jnp.dot(x_flat, w_block, preferred_element_type=jnp.float32)
        label_hit = col_ids == (label_flat - offset)[:, None]
        probs = jnp.exp(logits - row_max[:, None]) / row_sum[:, None]
        grad_logits = ((probs - label_hit.astype(jnp.float32)) / TOKENS).astype(jnp.bfloat16)
        grad_block = jnp.dot(x_flat.T, grad_logits, preferred_element_type=jnp.float32).astype(jnp.bfloat16)
        dx_acc = dx_acc + jnp.dot(grad_logits, w_block.T, preferred_element_type=jnp.float32)
        return dx_acc, grad_block

    dx_init = jnp.zeros((2 * TOKENS, HIDDEN), jnp.float32)
    dx_sum, grad_blocks = lax.scan(block_grad, dx_init, (w_blocks, offsets))
    grad_w = grad_blocks.transpose(1, 0, 2).reshape(HIDDEN, VOCAB)
    grad_x = dx_sum.astype(jnp.bfloat16)
    return losses, grad_w, grad_x[:TOKENS], grad_x[TOKENS:]
```

```python
import functools
import jax
import jax.numpy as jnp
from jax import lax
from jax.experimental import pallas as pl
from jax.experimental.pallas import tpu as pltpu
from jax.sharding import PartitionSpec as P

MESH = pl.DeviceIdType.MESH
F32, BF16 = jnp.float32, jnp.bfloat16
NT = 512
NS = 6
LOW = -3.0e38
VMEM = 63 * 2**20


def peer(me, chips, dr, flip):
    chip, core = me // 2, me % 2
    other = (1 - core) if flip else core
    return lax.rem(chip + dr, chips) * 2 + other


def ring_peers(me, chips):
    return peer(me, chips, 1, False), peer(me, chips, chips - 1, False), peer(me, chips, 0, True)


def k1_kernel(n, xa, xb, lab, w, z_out, xt_out, lcol_out, lab_out, loss_out,
              xs, xc, ws, zb0, zb1, mc, sc, tc, lc, mm, ss, tt, labin, labrel, st, stin, lrow, lossb,
              wsem, zsem, lsem, xsend, xrecv, labsend, labrecv, stsend, strecv):
    me = lax.axis_index("tp")
    chips = n // 2
    tok = xa.shape[0]
    cols = w.shape[1]
    tiles = cols // NT
    per = tiles // NS
    wide = NT * NS
    rows = 4 * tok
    half = tok // 2
    right, left, partner = ring_peers(me, chips)
    others = [(dr, f) for dr in range(chips) for f in (False, True) if dr or f]
    lo, hi, both, far = pl.ds(0, tok), pl.ds(tok, tok), pl.ds(0, 2 * tok), pl.ds(2 * tok, 2 * tok)
    lo0, lo1 = pl.ds(0, half), pl.ds(half, half)

    def rcopy(src, dst, k, dev):
        return pltpu.make_async_remote_copy(src_ref=src, dst_ref=dst, send_sem=xsend.at[k],
                                            recv_sem=xrecv.at[k], device_id={"tp": dev}, device_id_type=MESH)

    def to_all(src, dst, send, recv):
        made = []
        for dr, f in others:
            slot = ((chips - dr) % chips) * 2 + int(f)
            made.append(pltpu.make_async_remote_copy(src_ref=src, dst_ref=dst(slot), send_sem=send.at[slot], recv_sem=recv.at[slot],
                                                     device_id={"tp": peer(me, chips, dr, f)}, device_id_type=MESH))
        return made

    wcopy = [pltpu.make_async_copy(w.at[:, pl.ds(j * wide, wide)], ws.at[:, pl.ds(j * wide, wide)], wsem.at[j]) for j in range(per)]
    la = pltpu.make_async_copy(xa, xs.at[0, lo], lsem.at[0])
    lb = pltpu.make_async_copy(xb, xs.at[0, hi], lsem.at[1])
    ll = pltpu.make_async_copy(lab, labin.at[0], lsem.at[2])
    la.start()
    lb.start()
    ll.start()
    for c in wcopy:
        c.start()

    barrier = pltpu.get_barrier_semaphore()
    for dr, f in others:
        pl.semaphore_signal(barrier, inc=1, device_id={"tp": peer(me, chips, dr, f)}, device_id_type=MESH)
    la.wait()
    lb.wait()
    ll.wait()
    pl.semaphore_wait(barrier, n - 1)

    own_a, own_b = xs.at[0, lo], xs.at[0, hi]
    c_p = rcopy(xs.at[0, both], xs.at[0, far], 0, partner)
    c_3a = rcopy(own_a, xs.at[1, hi], 1, right)
    c_1a = rcopy(own_a, xs.at[1, lo], 2, left)
    c_3b = rcopy(own_b, xs.at[2, hi], 3, right)
    c_1b = rcopy(own_b, xs.at[2, lo], 4, left)
    c_f3a = rcopy(xs.at[1, pl.ds(tok, half)], xs.at[3, lo0], 5, right)
    c_f1a = rcopy(xs.at[1, lo1], xs.at[3, lo1], 6, left)
    c_f3b = rcopy(xs.at[2, pl.ds(tok, half)], xs.at[3, pl.ds(tok, half)], 7, right)
    c_f1b = rcopy(xs.at[2, lo1], xs.at[3, pl.ds(tok + half, half)], 8, left)
    c_d = [None] + [rcopy(xs.at[g, both], xs.at[g, far], 8 + g, partner) for g in (1, 2, 3)]
    c_lab = to_all(labin.at[0], lambda slot: labin.at[slot], labsend, labrecv)
    for c in c_lab + [c_p, c_3a, c_1a, c_3b, c_1b]:
        c.start()

    lane = lax.broadcasted_iota(jnp.int32, (2 * tok, 128), 1)
    shift = me * cols

    def put_labels(slot):
        r, f = slot // 2, slot % 2
        t = jnp.broadcast_to(labin[slot, 0:1, :], (2 * tok, 128)).T - lane - shift
        at = f * 2 * tok
        if r in (0, 2):
            labrel[{0: 0, 2: 3}[r], at:at + 2 * tok] = t
        else:
            o = at + (0 if r == 1 else tok)
            labrel[1, o:o + tok] = t[:tok]
            labrel[2, o:o + tok] = t[tok:]

    put_labels(0)
    c_p.wait()
    for c in c_lab:
        c.wait()
    for slot in range(1, n):
        put_labels(slot)

    def z_copy(g, zb):
        q = 0 if zb is zb0 else 1
        return pltpu.make_async_copy(zb, z_out.at[g, q], zsem.at[q])

    def epilogue(z, base):
        for r0 in range(0, rows, 32):
            rs = pl.ds(r0, 32)
            zc = [z[rs, k * 128:(k + 1) * 128] for k in range(NT // 128)]
            m_old = mc[rs]
            lr = lc[rs]
            m_new = functools.reduce(jnp.maximum, zc, m_old)
            mc[rs] = m_new
            s = sc[rs] * jnp.exp(m_old - m_new)
            sc[rs] = s + functools.reduce(jnp.add, [jnp.exp(c - m_new) for c in zc])
            tc[rs] = tc[rs] + functools.reduce(jnp.add, [jnp.where(lr == base + k * 128, c, 0.0) for k, c in enumerate(zc)])

    def half_step(g, q, zb, zprev):
        for t in range(NS):
            if t:
                epilogue(zb.at[t - 1], (q * NS + t - 1) * NT)
            elif q:
                epilogue(zprev.at[NS - 1], (NS - 1) * NT)
            zb[t] = jnp.dot(xc[...], ws[:, (q * NS + t) * NT:(q * NS + t + 1) * NT], preferred_element_type=F32)

    def step(g, _):
        for ev, fn in events.items():
            if ev % 2 == 0:
                pl.when(g == ev // 2)(fn)
        xc[...] = xs[g]
        lc[...] = labrel[g]
        mc[...] = jnp.full((rows, 128), LOW, F32)
        sc[...] = jnp.zeros((rows, 128), F32)
        tc[...] = jnp.zeros((rows, 128), F32)

        @pl.when(g == 0)
        def _():
            wcopy[0].wait()

        @pl.when(g >= 1)
        def _():
            z_copy(g - 1, zb0).wait()

        half_step(g, 0, zb0, zb1)
        for ev, fn in events.items():
            if ev % 2 == 1:
                pl.when(g == ev // 2)(fn)

        @pl.when(g == 0)
        def _():
            wcopy[1].wait()

        @pl.when(g >= 1)
        def _():
            z_copy(g - 1, zb1).wait()

        z_copy(g, zb0).start()
        half_step(g, 1, zb1, zb0)
        z_copy(g, zb1).start()
        epilogue(zb1.at[NS - 1], (tiles - 1) * NT)
        mm[g] = mc[...]
        ss[g] = sc[...]
        tt[g] = tc[...]
        return 0

    def ev_a():
        c_3a.wait_recv()
        c_1a.wait_recv()
        c_d[1].start()
        c_f3a.start()
        c_f1a.start()

    def ev_a2():
        c_d[1].wait_recv()

    def ev_b():
        c_3b.wait_recv()
        c_1b.wait_recv()
        c_d[2].start()
        c_f3b.start()
        c_f1b.start()

    def ev_b2():
        c_d[2].wait_recv()

    def ev_f():
        for c in (c_f3a, c_f1a, c_f3b, c_f1b):
            c.wait_recv()
        c_d[3].start()

    def ev_f2():
        c_d[3].wait_recv()

    events = {1: ev_a, 2: ev_a2, 3: ev_b, 4: ev_b2, 5: ev_f, 6: ev_f2}
    lax.fori_loop(0, 4, step, 0)

    def rows_of(ref, r, f):
        at = f * 2 * tok
        if r in (0, 2):
            return ref[{0: 0, 2: 3}[r], at:at + 2 * tok]
        o = at + (0 if r == 1 else tok)
        return jnp.concatenate([ref[1, o:o + tok], ref[2, o:o + tok]], axis=0)

    for slot in range(n):
        r, f = slot // 2, slot % 2
        m, s, t = (rows_of(ref, r, f) for ref in (mm, ss, tt))
        m_row = jnp.max(m, axis=1, keepdims=True)
        s_row = jnp.sum(s * jnp.exp(m - m_row), axis=1, keepdims=True)
        t_row = jnp.sum(t, axis=1, keepdims=True)
        packed = jnp.where(lane == 0, m_row, jnp.where(lane == 1, s_row, t_row)).T
        row = peer(me, chips, r, bool(f))
        for k in range(3):
            st[k, pl.ds(row, 1)] = packed[k:k + 1]
    c_st = to_all(st, lambda slot: stin.at[me], stsend, strecv)
    for c in c_st:
        c.start()
    stin[me] = st[...]
    hid = xs.shape[2]
    def tr(h, _):
        hs = pl.ds(pl.multiple_of(h * 256, 256), 256)
        for g in range(4):
            ws[hs, g * rows:(g + 1) * rows] = xs[g, :, hs].T
        return 0
    lax.fori_loop(0, hid // 256, tr, 0)
    c_xt = pltpu.make_async_copy(ws.at[:, pl.ds(0, 4 * rows)], xt_out, lsem.at[0])
    c_xt.start()
    for c in c_st:
        c.wait()
    m_all = functools.reduce(jnp.maximum, [stin[d, 0] for d in range(n)])
    s_all = functools.reduce(jnp.add, [stin[d, 1] * jnp.exp(stin[d, 0] - m_all) for d in range(n)])
    t_all = functools.reduce(jnp.add, [stin[d, 2] for d in range(n)])
    lse = m_all + jnp.log(s_all)
    lrow[...] = lse
    tok_loss = lse - t_all
    la_s = jnp.sum(tok_loss[:, :tok], keepdims=True)
    lb_s = jnp.sum(tok_loss[:, tok:], keepdims=True)
    l2 = lax.broadcasted_iota(jnp.int32, (8, 128), 1)
    lossb[...] = jnp.where(l2 == 0, la_s, lb_s) * (1.0 / (tok * n))
    for slot in range(n):
        r, f = slot // 2, slot % 2
        row = peer(me, chips, r, bool(f))
        t = jnp.broadcast_to(lrow[pl.ds(row, 1)], (2 * tok, 128)).T
        at = f * 2 * tok
        if r in (0, 2):
            mm[{0: 0, 2: 3}[r], at:at + 2 * tok] = t
        else:
            o = at + (0 if r == 1 else tok)
            mm[1, o:o + tok] = t[:tok]
            mm[2, o:o + tok] = t[tok:]
    outs = [pltpu.make_async_copy(mm, lcol_out, lsem.at[1]), pltpu.make_async_copy(labrel, lab_out, lsem.at[2]),
            pltpu.make_async_copy(lossb, loss_out, lsem.at[3])]
    for c in outs:
        c.start()
    for c in outs:
        c.wait()
    c_xt.wait()
    z_copy(3, zb0).wait()
    z_copy(3, zb1).wait()
    for c in (c_3a, c_1a, c_3b, c_1b, c_f3a, c_f1a, c_f3b, c_f1b, c_d[1], c_d[2], c_d[3]):
        c.wait_send()


def k1(n, xa, xb, la, lb, w):
    tok, hid = xa.shape
    cols = w.shape[1]
    tiles = cols // NT
    rows = 4 * tok
    lab = jnp.broadcast_to(jnp.concatenate([la, lb])[None, :], (8, 2 * tok))
    any_ = pl.BlockSpec(memory_space=pltpu.MemorySpace.HBM)
    return pl.pallas_call(
        functools.partial(k1_kernel, n),
        out_shape=[jax.ShapeDtypeStruct((4, tiles // NS, NS, rows, NT), F32), jax.ShapeDtypeStruct((hid, 4 * rows), BF16),
                   jax.ShapeDtypeStruct((4, rows, 128), F32), jax.ShapeDtypeStruct((4, rows, 128), jnp.int32),
                   jax.ShapeDtypeStruct((8, 128), F32)],
        in_specs=[any_] * 4,
        out_specs=[any_] * 5,
        scratch_shapes=[
            pltpu.VMEM((4, rows, hid), BF16), pltpu.VMEM((rows, hid), BF16), pltpu.VMEM((hid, cols), BF16),
            pltpu.VMEM((NS, rows, NT), F32), pltpu.VMEM((NS, rows, NT), F32), pltpu.VMEM((rows, 128), F32), pltpu.VMEM((rows, 128), F32), pltpu.VMEM((rows, 128), F32), pltpu.VMEM((rows, 128), jnp.int32), pltpu.VMEM((4, rows, 128), F32), pltpu.VMEM((4, rows, 128), F32),
            pltpu.VMEM((4, rows, 128), F32), pltpu.VMEM((n, 8, 2 * tok), jnp.int32), pltpu.VMEM((4, rows, 128), jnp.int32),
            pltpu.VMEM((3, n, 2 * tok), F32), pltpu.VMEM((n, 3, n, 2 * tok), F32), pltpu.VMEM((n, 2 * tok), F32), pltpu.VMEM((8, 128), F32),
            pltpu.SemaphoreType.DMA((tiles // NS,)), pltpu.SemaphoreType.DMA((2,)), pltpu.SemaphoreType.DMA((4,)),
            pltpu.SemaphoreType.DMA((12,)), pltpu.SemaphoreType.DMA((12,)), pltpu.SemaphoreType.DMA((n,)), pltpu.SemaphoreType.DMA((n,)),
            pltpu.SemaphoreType.DMA((n,)), pltpu.SemaphoreType.DMA((n,)),
        ],
        compiler_params=pltpu.CompilerParams(collective_id=0, has_side_effects=True, vmem_limit_bytes=VMEM),
        name="gather_logits",
    )(xa, xb, lab, w)


HC = 512
ACCS = 3
PH, PC = 512, 1024


def k2_kernel(n, cover, z, lcol, lab, w, xt, dxa_out, dxb_out, g_out, dw_out,
              g, lv, bv, z4, w0, w1, xv, d0, d1, pr, acc, r1, r2, ob0, ob1, oa,
              zsem, wsem, lsem, gsem, osem, psend, precv, s1send, s1recv, s2send, s2recv, fsem):
    me = lax.axis_index("tp")
    chips = n // 2
    right, left, partner = ring_peers(me, chips)
    rows = z.shape[3]
    tok = rows // 4
    halves, sub = z.shape[1], z.shape[2]
    hid, cols = w.shape
    chunks = hid // HC
    zn = 4 * halves * sub // 3
    barrier = pltpu.get_barrier_semaphore()
    for dev in (right, left, partner):
        pl.semaphore_signal(barrier, inc=1, device_id={"tp": dev}, device_id_type=MESH)

    def z_load(i, slot):
        gi, rest = i // (halves * sub // 3), lax.rem(i, halves * sub // 3)
        q, t = rest // (sub // 3), lax.rem(rest, sub // 3)
        return pltpu.make_async_copy(z.at[gi, q, pl.ds(t * 3, 3)], z4.at[slot], zsem.at[slot])

    def w_load(k, buf):
        return pltpu.make_async_copy(w.at[pl.ds(pl.multiple_of(k * HC, HC), HC)], buf, wsem.at[0 if buf is w0 else 1])

    small = [pltpu.make_async_copy(lcol, lv, lsem.at[0]), pltpu.make_async_copy(lab, bv, lsem.at[1]),
             pltpu.make_async_copy(xt.at[pl.ds(0, xv.shape[0])], xv, lsem.at[2])]
    small[0].start()
    small[1].start()
    for i in range(3):
        z_load(jnp.int32(i), i).start()
    w_load(0, w0).start()
    w_load(1, w1).start()
    small[2].start()
    small[0].wait()
    small[1].wait()
    inv = 1.0 / (tok * n)

    def soft(i, _):
        slot = lax.rem(i, 4)

        @pl.when(i + 3 < zn)
        def _():
            z_load(i + 3, lax.rem(i + 3, 4)).start()

        z_load(i, slot).wait()
        gi, rest = i // (halves * sub // 3), lax.rem(i, halves * sub // 3)
        for r0 in range(0, rows, 32):
            rs = pl.ds(r0, 32)
            lse = lv[gi, rs]
            lr = bv[gi, rs] - rest * (3 * NT)
            for t in range(3):
                out = []
                for k in range(NT // 128):
                    p = jnp.exp(z4[slot, t, rs, k * 128:(k + 1) * 128] - lse)
                    out.append((jnp.where(lr == t * NT + k * 128, p - 1.0, p) * inv).astype(BF16))
                g[pl.ds(pl.multiple_of(gi * rows + r0, 32), 32), pl.ds(pl.multiple_of(rest * (3 * NT) + t * NT, NT), NT)] = jnp.concatenate(out, axis=1)
        return 0

    lax.fori_loop(0, zn, soft, 0)
    c_g = pltpu.make_async_copy(g, g_out, gsem)
    c_g.start()
    small[2].wait()
    pl.semaphore_wait(barrier, 3)

    def remote(src, dst, ss, rs, dev):
        return pltpu.make_async_remote_copy(src_ref=src, dst_ref=dst, send_sem=ss, recv_sem=rs,
                                            device_id={"tp": dev}, device_id_type=MESH)

    lo, hi = pl.ds(0, tok), pl.ds(tok, tok)

    def pair(c, d):
        return remote(d.at[:, pl.ds(2 * tok, 2 * tok)], pr.at[c], psend.at[c], precv.at[c], partner)

    def first(c):
        a = acc.at[lax.rem(c, ACCS)]
        return [remote(a.at[3, lo], r1.at[c, 0], s1send.at[c, 0], s1recv.at[c, 0], right),
                remote(a.at[3, hi], r1.at[c, 1], s1send.at[c, 1], s1recv.at[c, 1], left),
                remote(a.at[2, lo], r2.at[c, 1], s2send.at[c, 1], s2recv.at[c, 1], right),
                remote(a.at[1, hi], r2.at[c, 2], s2send.at[c, 2], s2recv.at[c, 2], left)]

    def second(c):
        a = acc.at[lax.rem(c, ACCS)]
        return [remote(a.at[1, lo], r2.at[c, 0], s2send.at[c, 0], s2recv.at[c, 0], right),
                remote(a.at[2, hi], r2.at[c, 3], s2send.at[c, 3], s2recv.at[c, 3], left)]

    def do_first(c, d):
        pair(c, d).wait_recv()
        for b in range(4):
            acc[lax.rem(c, ACCS), b] = d[b, 0:2 * tok] + pr[c, b]
        for cp in first(c):
            cp.start()

    def do_second(c):
        f = first(c)
        f[0].wait_recv()
        f[1].wait_recv()
        s = lax.rem(c, ACCS)
        acc[s, 1, 0:tok] = acc[s, 1, 0:tok] + r1[c, 0]
        acc[s, 2, tok:] = acc[s, 2, tok:] + r1[c, 1]
        for cp in second(c):
            cp.start()

    def do_last(c):
        f, e = first(c), second(c)
        for cp in f[2:] + e:
            cp.wait_recv()
        s = lax.rem(c, ACCS)
        hs = pl.ds(pl.multiple_of(c * HC, HC), HC)
        oa[0:tok, hs] = (acc[s, 0, 0:tok] + (r2[c, 0] + r2[c, 2])).astype(BF16)
        oa[tok:, hs] = (acc[s, 0, tok:] + (r2[c, 1] + r2[c, 3])).astype(BF16)
        for cp in f + e:
            cp.wait_send()

    pcs = cols // PC

    def dw_copy(p, ob):
        hb, cb = p // pcs, lax.rem(p, pcs)
        return pltpu.make_async_copy(ob, dw_out.at[pl.ds(pl.multiple_of(hb * PH, PH), PH), pl.ds(pl.multiple_of(cb * PC, PC), PC)],
                                     osem.at[0 if ob is ob0 else 1])

    def dw_dot(p, ob):
        hb, cb = p // pcs, lax.rem(p, pcs)
        ob[...] = jnp.dot(xv[pl.ds(pl.multiple_of(hb * PH, PH), PH)], g[:, pl.ds(pl.multiple_of(cb * PC, PC), PC)],
                          preferred_element_type=F32).astype(BF16)

    obs = (ob0, ob1)

    def half(it, wb, d, dprev):
        w_load(it, wb).wait()

        @pl.when(it >= 2)
        def _():
            pair(it - 2, d).wait_send()

        d[...] = lax.dot_general(g[...], wb[...], (((1,), (1,)), ((), ())), preferred_element_type=F32).reshape(4, rows, HC)
        pair(it, d).start()

        @pl.when(it + 2 < chunks)
        def _():
            w_load(it + 2, wb).start()

        @pl.when(it >= 1)
        def _():
            do_second(it - 1)
            for i, ob in enumerate(obs):
                dw_copy(2 * it - 2 + i, ob).wait()

        for i, ob in enumerate(obs):
            dw_dot(2 * it + i, ob)
        for i, ob in enumerate(obs):
            dw_copy(2 * it + i, ob).start()
        do_first(it, d)

        @pl.when(it >= 2)
        def _():
            do_last(it - 2)

    def step(i2, _):
        half(2 * i2, w0, d0, d1)
        half(2 * i2 + 1, w1, d1, d0)
        return 0

    lax.fori_loop(0, chunks // 2, step, 0)
    end = jnp.int32(chunks - 1)

    def two(i, _):
        p = 2 * chunks + 2 * i
        for j, ob in enumerate(obs):
            dw_copy(p - 2 + j, ob).wait()
        for j, ob in enumerate(obs):
            dw_dot(p + j, ob)
        for j, ob in enumerate(obs):
            dw_copy(p + j, ob).start()

        @pl.when(i == 1)
        def _():
            do_second(end)
            do_last(end - 1)
        return 0

    lax.fori_loop(0, cover // 2 - chunks, two, 0)
    do_last(end)
    outs = [pltpu.make_async_copy(oa.at[lo], dxa_out, fsem.at[0]), pltpu.make_async_copy(oa.at[hi], dxb_out, fsem.at[1])]
    for c in outs:
        c.start()
    pair(chunks - 2, d0).wait_send()
    pair(chunks - 1, d1).wait_send()
    dw_copy(cover - 2, ob0).wait()
    dw_copy(cover - 1, ob1).wait()
    c_g.wait()
    for c in outs:
        c.wait()


def k2(n, cover, z, lcol, lab, w, xt):
    hid, cols = w.shape
    rows = z.shape[3]
    tok = rows // 4
    chunks = hid // HC
    part = cover // (cols // PC) * PH
    hbm = pl.BlockSpec(memory_space=pltpu.MemorySpace.HBM)
    dma = pltpu.SemaphoreType.DMA
    return pl.pallas_call(
        functools.partial(k2_kernel, n, cover),
        out_shape=[jax.ShapeDtypeStruct((tok, hid), BF16), jax.ShapeDtypeStruct((tok, hid), BF16),
                   jax.ShapeDtypeStruct((4 * rows, cols), BF16), jax.ShapeDtypeStruct((part, cols), BF16)],
        in_specs=[hbm] * 5,
        out_specs=[hbm] * 4,
        scratch_shapes=[
            pltpu.VMEM((4 * rows, cols), BF16), pltpu.VMEM((4, rows, 128), F32), pltpu.VMEM((4, rows, 128), jnp.int32),
            pltpu.VMEM((4, 3, rows, NT), F32), pltpu.VMEM((HC, cols), BF16), pltpu.VMEM((HC, cols), BF16),
            pltpu.VMEM((part, 4 * rows), BF16), pltpu.VMEM((4, rows, HC), F32), pltpu.VMEM((4, rows, HC), F32),
            pltpu.VMEM((chunks, 4, 2 * tok, HC), F32), pltpu.VMEM((ACCS, 4, 2 * tok, HC), F32),
            pltpu.VMEM((chunks, 2, tok, HC), F32), pltpu.VMEM((chunks, 4, tok, HC), F32),
            pltpu.VMEM((PH, PC), BF16), pltpu.VMEM((PH, PC), BF16), pltpu.VMEM((2 * tok, hid), BF16),
            dma((4,)), dma((2,)), dma((3,)), dma(()), dma((2,)), dma((chunks,)), dma((chunks,)),
            dma((chunks, 2)), dma((chunks, 2)), dma((chunks, 4)), dma((chunks, 4)), dma((2,)),
        ],
        compiler_params=pltpu.CompilerParams(collective_id=1, has_side_effects=True, vmem_limit_bytes=VMEM),
        name="grad_x_scatter",
    )(z, lcol, lab, w, xt)


def k3_kernel(g, xt, part, out, gv, xv, ob0, ob1, cb0, cb1, gsem, xsem, osem, isem, psem):
    prows, cols = part.shape
    hid = out.shape[0]
    rest = hid - prows
    blocks = cols // PC
    nb = rest // PH
    nc = prows // PH

    def g_load(c):
        return pltpu.make_async_copy(g.at[:, pl.ds(c * PC, PC)], gv.at[:, pl.ds(c * PC, PC)], gsem.at[c])

    cx = pltpu.make_async_copy(xt.at[pl.ds(prows, rest)], xv, xsem)
    cx.start()
    g_load(0).start()

    def tile(ref, r, c):
        return ref.at[pl.ds(r, PH), pl.ds(pl.multiple_of(c * PC, PC), PC)]

    def c_in(c, k, cb):
        return pltpu.make_async_copy(tile(part, k * PH, c), cb.at[k], isem.at[0 if cb is cb0 else 1, k])

    def c_out(c, k, cb):
        return pltpu.make_async_copy(cb.at[k], tile(out, k * PH, c), psem.at[0 if cb is cb0 else 1, k])

    def o_copy(c, k, ob):
        return pltpu.make_async_copy(ob.at[k], tile(out, prows + k * PH, c), osem.at[0 if ob is ob0 else 1, k])

    for k in range(nc):
        c_in(0, k, cb0).start()
    for c in range(1, blocks):
        g_load(c).start()
    cx.wait()

    def half(c, ob, cb, other):
        pltpu.make_async_copy(g.at[:, pl.ds(0, PC)], gv.at[:, pl.ds(0, PC)], gsem.at[c]).wait()

        @pl.when(c >= 2)
        def _():
            for k in range(nb):
                o_copy(c - 2, k, ob).wait()

        gs = pl.ds(pl.multiple_of(c * PC, PC), PC)
        for k in range(nb):
            ob[k] = jnp.dot(xv[k * PH:(k + 1) * PH], gv[:, gs], preferred_element_type=F32).astype(BF16)
        for k in range(nb):
            o_copy(c, k, ob).start()
        for k in range(nc):
            c_in(c, k, cb).wait()
            c_out(c, k, cb).start()

        @pl.when(c >= 1)
        def _():
            for k in range(nc):
                c_out(c - 1, k, other).wait()

        @pl.when(c + 1 < blocks)
        def _():
            for k in range(nc):
                c_in(c + 1, k, other).start()

    def step(i, _):
        half(2 * i, ob0, cb0, cb1)
        half(2 * i + 1, ob1, cb1, cb0)
        return 0

    lax.fori_loop(0, blocks // 2, step, 0)
    for k in range(nc):
        c_out(blocks - 1, k, cb1).wait()
    for k in range(nb):
        o_copy(blocks - 2, k, ob0).wait()
        o_copy(blocks - 1, k, ob1).wait()


def k3(g, xt, part):
    hid = xt.shape[0]
    rows, cols = g.shape
    prows = part.shape[0]
    rest = hid - prows
    hbm = pl.BlockSpec(memory_space=pltpu.MemorySpace.HBM)
    dma = pltpu.SemaphoreType.DMA
    return pl.pallas_call(
        k3_kernel,
        out_shape=jax.ShapeDtypeStruct((hid, cols), BF16),
        in_specs=[hbm] * 3,
        out_specs=hbm,
        scratch_shapes=[
            pltpu.VMEM((rows, cols), BF16), pltpu.VMEM((rest, rows), BF16), pltpu.VMEM((rest // PH, PH, PC), BF16),
            pltpu.VMEM((rest // PH, PH, PC), BF16), pltpu.VMEM((prows // PH, PH, PC), BF16), pltpu.VMEM((prows // PH, PH, PC), BF16),
            dma((cols // PC,)), dma(()), dma((2, rest // PH)), dma((2, prows // PH)), dma((2, prows // PH)),
        ],
        compiler_params=pltpu.CompilerParams(vmem_limit_bytes=VMEM),
        name="grad_w_rest",
    )(g, xt, part)


def solution(mesh):
    n = mesh.shape["tp"]

    def local_step(x_a, x_b, labels_a, labels_b, w):
        z, xt, lcol, labrel, loss = k1(n, x_a, x_b, labels_a, labels_b, w)
        gxa, gxb, g, part = k2(n, 18, z, lcol, labrel, w, xt)
        return loss[0, :2], k3(g, xt, part), gxa, gxb

    row_spec = P(("dp", "tp"), None)
    label_spec = P(("dp", "tp"))
    return jax.shard_map(local_step, mesh=mesh, in_specs=(row_spec, row_spec, label_spec, label_spec, P(None, "tp")), out_specs=(P("dp"), P("dp", "tp"), row_spec, row_spec), check_vma=False)
```

```python
import math
import functools
import jax
import jax.numpy as jnp
from jax import lax
from jax.experimental import pallas as pl
from jax.experimental.pallas import tpu as pltpu
from jax.sharding import PartitionSpec as P

MESH = pl.DeviceIdType.MESH
F32, BF16 = jnp.float32, jnp.bfloat16
NT = 512
NS = 6
LOW = -3.0e38
VMEM = 63 * 2**20


def peer(me, chips, dr, flip):
    chip, core = me // 2, me % 2
    other = (1 - core) if flip else core
    return lax.rem(chip + dr, chips) * 2 + other


def ring_peers(me, chips):
    return peer(me, chips, 1, False), peer(me, chips, chips - 1, False), peer(me, chips, 0, True)


def k1_kernel(n, xa, xb, lab, w, z_out, xt_out, lcol_out, lab_out, loss_out,
              xs, xc, ws, zb0, zb1, mc, sc, tc, lc, mm, ss, tt, labin, labrel, st, stin, lrow, lossb,
              wsem, zsem, lsem, xsend, xrecv, labsend, labrecv, stsend, strecv):
    me = lax.axis_index("tp")
    chips = n // 2
    tok = xa.shape[0]
    cols = w.shape[1]
    tiles = cols // NT
    per = tiles // NS
    wide = NT * NS
    rows = 4 * tok
    half = tok // 2
    right, left, partner = ring_peers(me, chips)
    others = [(dr, f) for dr in range(chips) for f in (False, True) if dr or f]
    lo, hi, both, far = pl.ds(0, tok), pl.ds(tok, tok), pl.ds(0, 2 * tok), pl.ds(2 * tok, 2 * tok)
    lo0, lo1 = pl.ds(0, half), pl.ds(half, half)

    def rcopy(src, dst, k, dev):
        return pltpu.make_async_remote_copy(src_ref=src, dst_ref=dst, send_sem=xsend.at[k],
                                            recv_sem=xrecv.at[k], device_id={"tp": dev}, device_id_type=MESH)

    def to_all(src, dst, send, recv):
        made = []
        for dr, f in others:
            slot = ((chips - dr) % chips) * 2 + int(f)
            made.append(pltpu.make_async_remote_copy(src_ref=src, dst_ref=dst(slot), send_sem=send.at[slot], recv_sem=recv.at[slot],
                                                     device_id={"tp": peer(me, chips, dr, f)}, device_id_type=MESH))
        return made

    wcopy = [pltpu.make_async_copy(w.at[:, pl.ds(j * wide, wide)], ws.at[:, pl.ds(j * wide, wide)], wsem.at[j]) for j in range(per)]
    la = pltpu.make_async_copy(xa, xs.at[0, lo], lsem.at[0])
    lb = pltpu.make_async_copy(xb, xs.at[0, hi], lsem.at[1])
    ll = pltpu.make_async_copy(lab, labin.at[0], lsem.at[2])
    la.start()
    lb.start()
    ll.start()
    for c in wcopy:
        c.start()

    barrier = pltpu.get_barrier_semaphore()
    for dr, f in others:
        pl.semaphore_signal(barrier, inc=1, device_id={"tp": peer(me, chips, dr, f)}, device_id_type=MESH)
    la.wait()
    lb.wait()
    ll.wait()
    pl.semaphore_wait(barrier, n - 1)

    own_a, own_b = xs.at[0, lo], xs.at[0, hi]
    c_p = rcopy(xs.at[0, both], xs.at[0, far], 0, partner)
    c_3a = rcopy(own_a, xs.at[1, hi], 1, right)
    c_1a = rcopy(own_a, xs.at[1, lo], 2, left)
    c_3b = rcopy(own_b, xs.at[2, hi], 3, right)
    c_1b = rcopy(own_b, xs.at[2, lo], 4, left)
    c_f3a = rcopy(xs.at[1, pl.ds(tok, half)], xs.at[3, lo0], 5, right)
    c_f1a = rcopy(xs.at[1, lo1], xs.at[3, lo1], 6, left)
    c_f3b = rcopy(xs.at[2, pl.ds(tok, half)], xs.at[3, pl.ds(tok, half)], 7, right)
    c_f1b = rcopy(xs.at[2, lo1], xs.at[3, pl.ds(tok + half, half)], 8, left)
    c_d = [None] + [rcopy(xs.at[g, both], xs.at[g, far], 8 + g, partner) for g in (1, 2, 3)]
    c_lab = to_all(labin.at[0], lambda slot: labin.at[slot], labsend, labrecv)
    for c in c_lab + [c_p, c_3a, c_1a, c_3b, c_1b]:
        c.start()

    lane = lax.broadcasted_iota(jnp.int32, (2 * tok, 128), 1)
    shift = me * cols

    def put_labels(slot):
        r, f = slot // 2, slot % 2
        t = jnp.broadcast_to(labin[slot, 0:1, :], (2 * tok, 128)).T - lane - shift
        at = f * 2 * tok
        if r in (0, 2):
            labrel[{0: 0, 2: 3}[r], at:at + 2 * tok] = t
        else:
            o = at + (0 if r == 1 else tok)
            labrel[1, o:o + tok] = t[:tok]
            labrel[2, o:o + tok] = t[tok:]

    put_labels(0)
    c_p.wait()
    for c in c_lab:
        c.wait()
    for slot in range(1, n):
        put_labels(slot)

    def z_copy(g, zb):
        q = 0 if zb is zb0 else 1
        return pltpu.make_async_copy(zb, z_out.at[g, q], zsem.at[q])

    def epilogue(z, base):
        for r0 in range(0, rows, 32):
            rs = pl.ds(r0, 32)
            zc = [z[rs, k * 128:(k + 1) * 128] for k in range(NT // 128)]
            m_old = mc[rs]
            lr = lc[rs]
            m_new = functools.reduce(jnp.maximum, zc, m_old)
            mc[rs] = m_new
            s = sc[rs] * jnp.exp(m_old - m_new)
            sc[rs] = s + functools.reduce(jnp.add, [jnp.exp(c - m_new) for c in zc])
            tc[rs] = tc[rs] + functools.reduce(jnp.add, [jnp.where(lr == base + k * 128, c, 0.0) for k, c in enumerate(zc)])

    def half_step(g, q, zb, zprev):
        for t in range(NS):
            if t:
                epilogue(zb.at[t - 1], (q * NS + t - 1) * NT)
            elif q:
                epilogue(zprev.at[NS - 1], (NS - 1) * NT)
            if q and t == NS // 2:
                for ev, fn in enumerate(late):
                    pl.when(g == ev)(fn)
            zb[t] = jnp.dot(xc[...], ws[:, (q * NS + t) * NT:(q * NS + t + 1) * NT], preferred_element_type=F32)

    def step(g, _):
        for ev, fn in enumerate(early):
            pl.when(g == ev + 1)(fn)
        xc[...] = xs[g]
        lc[...] = labrel[g]
        mc[...] = jnp.full((rows, 128), LOW, F32)
        sc[...] = jnp.zeros((rows, 128), F32)
        tc[...] = jnp.zeros((rows, 128), F32)

        @pl.when(g == 0)
        def _():
            wcopy[0].wait()

        @pl.when(g >= 1)
        def _():
            z_copy(g - 1, zb0).wait()

        half_step(g, 0, zb0, zb1)

        @pl.when(g == 0)
        def _():
            wcopy[1].wait()

        @pl.when(g >= 1)
        def _():
            z_copy(g - 1, zb1).wait()

        z_copy(g, zb0).start()
        half_step(g, 1, zb1, zb0)
        z_copy(g, zb1).start()
        epilogue(zb1.at[NS - 1], (tiles - 1) * NT)
        mm[g] = mc[...]
        ss[g] = sc[...]
        tt[g] = tc[...]
        return 0

    def ev_a():
        c_3a.wait_recv()
        c_1a.wait_recv()
        c_d[1].start()
        c_f3a.start()
        c_f1a.start()

    def ev_a2():
        c_d[1].wait_recv()

    def ev_b():
        c_3b.wait_recv()
        c_1b.wait_recv()
        c_d[2].start()
        c_f3b.start()
        c_f1b.start()

    def ev_b2():
        c_d[2].wait_recv()

    def ev_f():
        for c in (c_f3a, c_f1a, c_f3b, c_f1b):
            c.wait_recv()
        c_d[3].start()

    def ev_f2():
        c_d[3].wait_recv()

    late, early = (ev_a, ev_b, ev_f), (ev_a2, ev_b2, ev_f2)
    lax.fori_loop(0, 4, step, 0)

    def rows_of(ref, r, f):
        at = f * 2 * tok
        if r in (0, 2):
            return ref[{0: 0, 2: 3}[r], at:at + 2 * tok]
        o = at + (0 if r == 1 else tok)
        return jnp.concatenate([ref[1, o:o + tok], ref[2, o:o + tok]], axis=0)

    for slot in range(n):
        r, f = slot // 2, slot % 2
        m, s, t = (rows_of(ref, r, f) for ref in (mm, ss, tt))
        m_row = jnp.max(m, axis=1, keepdims=True)
        s_row = jnp.sum(s * jnp.exp(m - m_row), axis=1, keepdims=True)
        t_row = jnp.sum(t, axis=1, keepdims=True)
        packed = jnp.where(lane == 0, m_row, jnp.where(lane == 1, s_row, t_row)).T
        row = peer(me, chips, r, bool(f))
        for k in range(3):
            st[k, pl.ds(row, 1)] = packed[k:k + 1]
    c_st = to_all(st, lambda slot: stin.at[me], stsend, strecv)
    for c in c_st:
        c.start()
    stin[me] = st[...]
    hid = xs.shape[2]
    def tr(h, _):
        hs = pl.ds(pl.multiple_of(h * 256, 256), 256)
        for g in range(4):
            ws[hs, g * rows:(g + 1) * rows] = xs[g, :, hs].T
        return 0
    lax.fori_loop(0, hid // 256, tr, 0)
    c_xt = pltpu.make_async_copy(ws.at[:, pl.ds(0, 4 * rows)], xt_out, lsem.at[0])
    c_xt.start()
    for c in c_st:
        c.wait()
    m_all = functools.reduce(jnp.maximum, [stin[d, 0] for d in range(n)])
    s_all = functools.reduce(jnp.add, [stin[d, 1] * jnp.exp(stin[d, 0] - m_all) for d in range(n)])
    t_all = functools.reduce(jnp.add, [stin[d, 2] for d in range(n)])
    lse = m_all + jnp.log(s_all)
    lrow[...] = lse
    tok_loss = lse - t_all
    la_s = jnp.sum(tok_loss[:, :tok], keepdims=True)
    lb_s = jnp.sum(tok_loss[:, tok:], keepdims=True)
    l2 = lax.broadcasted_iota(jnp.int32, (8, 128), 1)
    lossb[...] = jnp.where(l2 == 0, la_s, lb_s) * (1.0 / (tok * n))
    for slot in range(n):
        r, f = slot // 2, slot % 2
        row = peer(me, chips, r, bool(f))
        t = jnp.broadcast_to(lrow[pl.ds(row, 1)], (2 * tok, 128)).T
        at = f * 2 * tok
        if r in (0, 2):
            mm[{0: 0, 2: 3}[r], at:at + 2 * tok] = t
        else:
            o = at + (0 if r == 1 else tok)
            mm[1, o:o + tok] = t[:tok]
            mm[2, o:o + tok] = t[tok:]
    outs = [pltpu.make_async_copy(mm, lcol_out, lsem.at[1]), pltpu.make_async_copy(labrel, lab_out, lsem.at[2]),
            pltpu.make_async_copy(lossb, loss_out, lsem.at[3])]
    for c in outs:
        c.start()
    for c in outs:
        c.wait()
    c_xt.wait()
    z_copy(3, zb0).wait()
    z_copy(3, zb1).wait()
    for c in (c_3a, c_1a, c_3b, c_1b, c_f3a, c_f1a, c_f3b, c_f1b, c_d[1], c_d[2], c_d[3]):
        c.wait_send()


def k1(n, xa, xb, la, lb, w):
    tok, hid = xa.shape
    cols = w.shape[1]
    tiles = cols // NT
    rows = 4 * tok
    lab = jnp.broadcast_to(jnp.concatenate([la, lb])[None, :], (8, 2 * tok))
    any_ = pl.BlockSpec(memory_space=pltpu.MemorySpace.HBM)
    return pl.pallas_call(
        functools.partial(k1_kernel, n),
        out_shape=[jax.ShapeDtypeStruct((4, tiles // NS, NS, rows, NT), F32), jax.ShapeDtypeStruct((hid, 4 * rows), BF16),
                   jax.ShapeDtypeStruct((4, rows, 128), F32), jax.ShapeDtypeStruct((4, rows, 128), jnp.int32),
                   jax.ShapeDtypeStruct((8, 128), F32)],
        in_specs=[any_] * 4,
        out_specs=[any_] * 5,
        scratch_shapes=[
            pltpu.VMEM((4, rows, hid), BF16), pltpu.VMEM((rows, hid), BF16), pltpu.VMEM((hid, cols), BF16),
            pltpu.VMEM((NS, rows, NT), F32), pltpu.VMEM((NS, rows, NT), F32), pltpu.VMEM((rows, 128), F32), pltpu.VMEM((rows, 128), F32), pltpu.VMEM((rows, 128), F32), pltpu.VMEM((rows, 128), jnp.int32), pltpu.VMEM((4, rows, 128), F32), pltpu.VMEM((4, rows, 128), F32),
            pltpu.VMEM((4, rows, 128), F32), pltpu.VMEM((n, 8, 2 * tok), jnp.int32), pltpu.VMEM((4, rows, 128), jnp.int32),
            pltpu.VMEM((3, n, 2 * tok), F32), pltpu.VMEM((n, 3, n, 2 * tok), F32), pltpu.VMEM((n, 2 * tok), F32), pltpu.VMEM((8, 128), F32),
            pltpu.SemaphoreType.DMA((2,)), pltpu.SemaphoreType.DMA((2,)), pltpu.SemaphoreType.DMA((4,)),
            pltpu.SemaphoreType.DMA((12,)), pltpu.SemaphoreType.DMA((12,)), pltpu.SemaphoreType.DMA((n,)), pltpu.SemaphoreType.DMA((n,)),
            pltpu.SemaphoreType.DMA((n,)), pltpu.SemaphoreType.DMA((n,)),
        ],
        compiler_params=pltpu.CompilerParams(collective_id=0, has_side_effects=True, vmem_limit_bytes=VMEM),
        name="gather_logits",
    )(xa, xb, lab, w)


HC = 512
ACCS = 3
PH, PC = 512, 1024


def k2_kernel(n, cover, z, lcol, lab, w, xt, dx_out, g_out, dw_out,
              g, lv, bv, z4, w0, w1, xv, d0, d1, pr, acc, r1, r2, ob0, ob1, oa,
              zsem, wsem, lsem, gsem, osem, psend, precv, s1send, s1recv, s2send, s2recv, fsem):
    me = lax.axis_index("tp")
    chips = n // 2
    right, left, partner = ring_peers(me, chips)
    rows = z.shape[3]
    tok = rows // 4
    halves, sub = z.shape[1], z.shape[2]
    hid, cols = w.shape
    chunks = hid // HC
    zn = 4 * halves * sub // 3
    barrier = pltpu.get_barrier_semaphore()
    for dev in (right, left, partner):
        pl.semaphore_signal(barrier, inc=1, device_id={"tp": dev}, device_id_type=MESH)

    def z_load(i, slot):
        gi, rest = i // (halves * sub // 3), lax.rem(i, halves * sub // 3)
        q, t = rest // (sub // 3), lax.rem(rest, sub // 3)
        return pltpu.make_async_copy(z.at[gi, q, pl.ds(t * 3, 3)], z4.at[slot], zsem.at[slot])

    def w_load(k, buf):
        return pltpu.make_async_copy(w.at[pl.ds(pl.multiple_of(k * HC, HC), HC)], buf, wsem.at[0 if buf is w0 else 1])

    small = [pltpu.make_async_copy(lcol, lv, lsem.at[0]), pltpu.make_async_copy(lab, bv, lsem.at[1]),
             pltpu.make_async_copy(xt.at[pl.ds(0, xv.shape[0])], xv, lsem.at[2])]
    small[0].start()
    small[1].start()
    for i in range(3):
        z_load(jnp.int32(i), i).start()
    w_load(0, w0).start()
    w_load(1, w1).start()
    small[2].start()
    small[0].wait()
    small[1].wait()
    inv, log_t = 1.0 / (tok * n), math.log(tok * n)

    def soft(i, _):
        slot = lax.rem(i, 4)

        @pl.when(i + 3 < zn)
        def _():
            z_load(i + 3, lax.rem(i + 3, 4)).start()

        z_load(i, slot).wait()
        gi, rest = i // (halves * sub // 3), lax.rem(i, halves * sub // 3)
        for r0 in range(0, rows, 32):
            rs = pl.ds(r0, 32)
            lse = lv[gi, rs] + log_t
            lr = bv[gi, rs] - rest * (3 * NT)
            for t in range(3):
                out = []
                for k in range(NT // 128):
                    p = jnp.exp(z4[slot, t, rs, k * 128:(k + 1) * 128] - lse)
                    out.append(jnp.where(lr == t * NT + k * 128, p - inv, p).astype(BF16))
                g[pl.ds(pl.multiple_of(gi * rows + r0, 32), 32), pl.ds(pl.multiple_of(rest * (3 * NT) + t * NT, NT), NT)] = jnp.concatenate(out, axis=1)
        return 0

    lax.fori_loop(0, zn, soft, 0)
    c_g = pltpu.make_async_copy(g, g_out, gsem)
    c_g.start()
    small[2].wait()
    pl.semaphore_wait(barrier, 3)

    def remote(src, dst, ss, rs, dev):
        return pltpu.make_async_remote_copy(src_ref=src, dst_ref=dst, send_sem=ss, recv_sem=rs,
                                            device_id={"tp": dev}, device_id_type=MESH)

    lo, hi = pl.ds(0, tok), pl.ds(tok, tok)

    def pair(c, d):
        return remote(d.at[:, pl.ds(2 * tok, 2 * tok)], pr.at[c], psend.at[c], precv.at[c], partner)

    def first(c):
        a = acc.at[lax.rem(c, ACCS)]
        return [remote(a.at[3, lo], r1.at[c, 0], s1send.at[c, 0], s1recv.at[c, 0], right),
                remote(a.at[3, hi], r1.at[c, 1], s1send.at[c, 1], s1recv.at[c, 1], left),
                remote(a.at[2, lo], r2.at[c, 1], s2send.at[c, 1], s2recv.at[c, 1], right),
                remote(a.at[1, hi], r2.at[c, 2], s2send.at[c, 2], s2recv.at[c, 2], left)]

    def second(c):
        a = acc.at[lax.rem(c, ACCS)]
        return [remote(a.at[1, lo], r2.at[c, 0], s2send.at[c, 0], s2recv.at[c, 0], right),
                remote(a.at[2, hi], r2.at[c, 3], s2send.at[c, 3], s2recv.at[c, 3], left)]

    def do_first(c, d):
        pair(c, d).wait_recv()
        for b in range(4):
            acc[lax.rem(c, ACCS), b] = d[b, 0:2 * tok] + pr[c, b]
        for cp in first(c):
            cp.start()

    def do_second(c):
        f = first(c)
        f[0].wait_recv()
        f[1].wait_recv()
        s = lax.rem(c, ACCS)
        acc[s, 1, 0:tok] = acc[s, 1, 0:tok] + r1[c, 0]
        acc[s, 2, tok:] = acc[s, 2, tok:] + r1[c, 1]
        for cp in second(c):
            cp.start()

    def do_last(c):
        f, e = first(c), second(c)
        for cp in f[2:] + e:
            cp.wait_recv()
        s = lax.rem(c, ACCS)
        hs = pl.ds(pl.multiple_of(c * HC, HC), HC)
        oa[0:tok, hs] = (acc[s, 0, 0:tok] + (r2[c, 0] + r2[c, 2])).astype(BF16)
        oa[tok:, hs] = (acc[s, 0, tok:] + (r2[c, 1] + r2[c, 3])).astype(BF16)
        for cp in f + e:
            cp.wait_send()

    pcs = cols // PC

    def dw_copy(p, ob):
        hb, cb = p // pcs, lax.rem(p, pcs)
        return pltpu.make_async_copy(ob, dw_out.at[pl.ds(pl.multiple_of(hb * PH, PH), PH), pl.ds(pl.multiple_of(cb * PC, PC), PC)],
                                     osem.at[0 if ob is ob0 else 1])

    def dw_dot(p, ob):
        hb, cb = p // pcs, lax.rem(p, pcs)
        ob[...] = jnp.dot(xv[pl.ds(pl.multiple_of(hb * PH, PH), PH)], g[:, pl.ds(pl.multiple_of(cb * PC, PC), PC)],
                          preferred_element_type=F32).astype(BF16)

    obs = (ob0, ob1)

    def half(it, wb, d, dprev):
        w_load(it, wb).wait()

        @pl.when(it >= 2)
        def _():
            pair(it - 2, d).wait_send()

        d[...] = lax.dot_general(g[...], wb[...], (((1,), (1,)), ((), ())), preferred_element_type=F32).reshape(4, rows, HC)
        pair(it, d).start()

        @pl.when(it + 2 < chunks)
        def _():
            w_load(it + 2, wb).start()

        @pl.when(it >= 1)
        def _():
            do_second(it - 1)
            for i, ob in enumerate(obs):
                dw_copy(2 * it - 2 + i, ob).wait()

        for i, ob in enumerate(obs):
            dw_dot(2 * it + i, ob)
        for i, ob in enumerate(obs):
            dw_copy(2 * it + i, ob).start()
        do_first(it, d)

        @pl.when(it >= 2)
        def _():
            do_last(it - 2)

    def step(i2, _):
        half(2 * i2, w0, d0, d1)
        half(2 * i2 + 1, w1, d1, d0)
        return 0

    lax.fori_loop(0, chunks // 2, step, 0)
    end = jnp.int32(chunks - 1)

    def two(i, _):
        p = 2 * chunks + 2 * i
        for j, ob in enumerate(obs):
            dw_copy(p - 2 + j, ob).wait()
        for j, ob in enumerate(obs):
            dw_dot(p + j, ob)
        for j, ob in enumerate(obs):
            dw_copy(p + j, ob).start()

        @pl.when(i == 1)
        def _():
            do_second(end)
            do_last(end - 1)
        return 0

    lax.fori_loop(0, cover // 2 - chunks, two, 0)
    do_last(end)
    c_dx = pltpu.make_async_copy(oa, dx_out, fsem)
    c_dx.start()
    pair(chunks - 2, d0).wait_send()
    pair(chunks - 1, d1).wait_send()
    dw_copy(cover - 2, ob0).wait()
    dw_copy(cover - 1, ob1).wait()
    c_g.wait()
    c_dx.wait()


def k2(n, cover, z, lcol, lab, w, xt):
    hid, cols = w.shape
    rows = z.shape[3]
    tok = rows // 4
    chunks = hid // HC
    part = cover // (cols // PC) * PH
    hbm = pl.BlockSpec(memory_space=pltpu.MemorySpace.HBM)
    dma = pltpu.SemaphoreType.DMA
    return pl.pallas_call(
        functools.partial(k2_kernel, n, cover),
        out_shape=[jax.ShapeDtypeStruct((2 * tok, hid), BF16),
                   jax.ShapeDtypeStruct((4 * rows, cols), BF16), jax.ShapeDtypeStruct((part, cols), BF16)],
        in_specs=[hbm] * 5,
        out_specs=[hbm] * 3,
        scratch_shapes=[
            pltpu.VMEM((4 * rows, cols), BF16), pltpu.VMEM((4, rows, 128), F32), pltpu.VMEM((4, rows, 128), jnp.int32),
            pltpu.VMEM((4, 3, rows, NT), F32), pltpu.VMEM((HC, cols), BF16), pltpu.VMEM((HC, cols), BF16),
            pltpu.VMEM((part, 4 * rows), BF16), pltpu.VMEM((4, rows, HC), F32), pltpu.VMEM((4, rows, HC), F32),
            pltpu.VMEM((chunks, 4, 2 * tok, HC), F32), pltpu.VMEM((ACCS, 4, 2 * tok, HC), F32),
            pltpu.VMEM((chunks, 2, tok, HC), F32), pltpu.VMEM((chunks, 4, tok, HC), F32),
            pltpu.VMEM((PH, PC), BF16), pltpu.VMEM((PH, PC), BF16), pltpu.VMEM((2 * tok, hid), BF16),
            dma((4,)), dma((2,)), dma((3,)), dma(()), dma((2,)), dma((chunks,)), dma((chunks,)),
            dma((chunks, 2)), dma((chunks, 2)), dma((chunks, 4)), dma((chunks, 4)), dma(()),
        ],
        compiler_params=pltpu.CompilerParams(collective_id=1, has_side_effects=True, vmem_limit_bytes=VMEM),
        name="grad_x_scatter",
    )(z, lcol, lab, w, xt)


def k3_kernel(g, xt, part, dx, loss, loss_out, out, dxa_out, dxb_out, dxv, dsem, gv, xv, ob0, ob1, cb0, cb1, gsem, xsem, osem, isem, psem):
    prows, cols = part.shape
    hid = out.shape[0]
    rest = hid - prows
    blocks = cols // PC
    nb = rest // PH
    nc = prows // PH

    def g_load(c):
        return pltpu.make_async_copy(g.at[:, pl.ds(c * PC, PC)], gv.at[:, pl.ds(c * PC, PC)], gsem.at[c])

    loss_out[0] = loss[0, 0]
    loss_out[1] = loss[0, 1]
    tok = dxa_out.shape[0]
    c_dx = pltpu.make_async_copy(dx, dxv, dsem.at[0])
    d_out = [pltpu.make_async_copy(dxv.at[pl.ds(i * tok, tok)], o, dsem.at[1 + i]) for i, o in enumerate((dxa_out, dxb_out))]
    cx = pltpu.make_async_copy(xt.at[pl.ds(prows, rest)], xv, xsem)
    cx.start()
    g_load(0).start()

    def tile(ref, r, c):
        return ref.at[pl.ds(r, PH), pl.ds(pl.multiple_of(c * PC, PC), PC)]

    def c_in(c, k, cb):
        return pltpu.make_async_copy(tile(part, k * PH, c), cb.at[k], isem.at[0 if cb is cb0 else 1, k])

    def c_out(c, k, cb):
        return pltpu.make_async_copy(cb.at[k], tile(out, k * PH, c), psem.at[0 if cb is cb0 else 1, k])

    def o_copy(c, k, ob):
        return pltpu.make_async_copy(ob.at[k], tile(out, prows + k * PH, c), osem.at[0 if ob is ob0 else 1, k])

    for k in range(nc):
        c_in(0, k, cb0).start()
    for c in range(1, blocks):
        g_load(c).start()
    c_dx.start()
    cx.wait()

    def half(c, ob, cb, other):
        pltpu.make_async_copy(g.at[:, pl.ds(0, PC)], gv.at[:, pl.ds(0, PC)], gsem.at[c]).wait()

        @pl.when(c >= 2)
        def _():
            for k in range(nb):
                o_copy(c - 2, k, ob).wait()

        gs = pl.ds(pl.multiple_of(c * PC, PC), PC)
        for k in range(nb):
            ob[k] = jnp.dot(xv[k * PH:(k + 1) * PH], gv[:, gs], preferred_element_type=F32).astype(BF16)
        for k in range(nb):
            o_copy(c, k, ob).start()
        for k in range(nc):
            c_in(c, k, cb).wait()
            c_out(c, k, cb).start()

        @pl.when(c >= 1)
        def _():
            for k in range(nc):
                c_out(c - 1, k, other).wait()

        @pl.when(c + 1 < blocks)
        def _():
            for k in range(nc):
                c_in(c + 1, k, other).start()

    def step(i, _):
        @pl.when(i == 1)
        def _():
            c_dx.wait()
            for c in d_out:
                c.start()

        half(2 * i, ob0, cb0, cb1)
        half(2 * i + 1, ob1, cb1, cb0)
        return 0

    lax.fori_loop(0, blocks // 2, step, 0)
    for k in range(nc):
        c_out(blocks - 1, k, cb1).wait()
    for k in range(nb):
        o_copy(blocks - 2, k, ob0).wait()
        o_copy(blocks - 1, k, ob1).wait()
    for c in d_out:
        c.wait()


def k3(g, xt, part, dx, loss):
    hid = xt.shape[0]
    rows, cols = g.shape
    prows = part.shape[0]
    rest = hid - prows
    hbm = pl.BlockSpec(memory_space=pltpu.MemorySpace.HBM)
    dma = pltpu.SemaphoreType.DMA
    return pl.pallas_call(
        k3_kernel,
        out_shape=[jax.ShapeDtypeStruct((2,), F32), jax.ShapeDtypeStruct((hid, cols), BF16)] + [jax.ShapeDtypeStruct((dx.shape[0] // 2, hid), BF16)] * 2,
        in_specs=[hbm] * 4 + [pl.BlockSpec(memory_space=pltpu.VMEM)],
        out_specs=[pl.BlockSpec(memory_space=pltpu.SMEM)] + [hbm] * 3,
        scratch_shapes=[
            pltpu.VMEM(dx.shape, BF16), dma((3,)),
            pltpu.VMEM((rows, cols), BF16), pltpu.VMEM((rest, rows), BF16), pltpu.VMEM((rest // PH, PH, PC), BF16),
            pltpu.VMEM((rest // PH, PH, PC), BF16), pltpu.VMEM((prows // PH, PH, PC), BF16), pltpu.VMEM((prows // PH, PH, PC), BF16),
            dma((cols // PC,)), dma(()), dma((2, rest // PH)), dma((2, prows // PH)), dma((2, prows // PH)),
        ],
        compiler_params=pltpu.CompilerParams(vmem_limit_bytes=VMEM),
        name="grad_w_rest",
    )(g, xt, part, dx, loss)


def solution(mesh):
    n = mesh.shape["tp"]

    def local_step(x_a, x_b, labels_a, labels_b, w):
        z, xt, lcol, labrel, loss = k1(n, x_a, x_b, labels_a, labels_b, w)
        dx, g, part = k2(n, 18, z, lcol, labrel, w, xt)
        return tuple(k3(g, xt, part, dx, loss))

    row_spec = P(("dp", "tp"), None)
    label_spec = P(("dp", "tp"))
    return jax.shard_map(local_step, mesh=mesh, in_specs=(row_spec, row_spec, label_spec, label_spec, P(None, "tp")), out_specs=(P("dp"), P("dp", "tp"), row_spec, row_spec), check_vma=False)
```
